32 devices in a mesh: slides: 2 (over y), row: 16 (over z, x, core).
Axes of the slice: x: 2, y: 2, z: 4, core: 2. Of those that a mesh axis runs over, the one named last changes fastest.
Arguments:
- slide_pixels: bfloat16 [2048, 16384], P(('slides', 'row')), parts along dimension 0, may hold values from -6 to 6
- tissue_mask: int32 [64, 8], P(('slides', 'row')), parts along dimension 0, may hold values from 0 to 1, as said below
- conv_weight: bfloat16 [3, 3, 64, 64], replicated, may hold values from -0.25 to 0.25
- conv_bias: bfloat16 [64], replicated, may hold values from -3 to 3
Outputs:
- packed_tiles: bfloat16 [256, 32, 2048], P(('slides', 'row')), parts along dimension 0
The draws below stay inside these ranges and needn't reach their ends.
There are 2 independent parts, one for each index of `slides`. The reference program is written for one: setup_inputs(seed, part) draws one part's arguments, and reference() takes and returns one part's arrays. A program takes and returns all parts, laid end to end along the dimension named above; an argument that names none is the same for every part. Nothing has to cross between parts.
Inputs may be any that keep to these rules, and one draw needn't show every extreme that they name: `tissue_mask`: exactly 128 tiles hold tissue. For every s from 1 to 15, the first s * 2 tile rows hold s * 8 + e tissue tiles with e between 0 and 2; e = 2 occurs in every draw. For every such s, some column holds tissue in both tile row s * 2 - 1 and tile row s * 2.
All inputs are finite; a program needn't handle non-finite values.
Results may differ from the reference program's by a relative error of at most 0.001.
Values may be sent and summed in bfloat16 or wider, within the bound.
A program may use at most 64 MiB of HBM per device.

```python
import jax
import jax.numpy as jnp
from jax import lax

CH = 64
SIDE = 32
SLOTS = 8
ROWS_DEV = 2
COLS = 8
SHIFT_MOST = 2
GRID_ROWS = 32
N_ROW = 16


def draw_tissue_mask(key, part):
    walk_key, first_key, order_key, column_key = jax.random.split(jax.random.fold_in(key, 7), 4)
    device_total = N_ROW
    reach_most = SHIFT_MOST
    drift_walk = jax.random.randint(walk_key, (device_total + 1,), 0, reach_most + 1)
    first_step = jax.random.randint(first_key, (), 1, device_total)
    step_index = jnp.arange(device_total + 1)
    drift_walk = jnp.where(step_index == first_step, reach_most, drift_walk)
    middle = device_total // 2
    in_window = (step_index >= middle - 2) & (step_index <= middle + 3)
    alternating = step_index % 2 * reach_most
    drift_walk = jnp.where(in_window, alternating, drift_walk)
    drift_walk = jnp.where((step_index == 0) | (step_index == device_total), 0, drift_walk)
    counts = SLOTS + drift_walk[1:] - drift_walk[:-1]
    tiles_band = ROWS_DEV * COLS
    boundary_cols = jax.random.randint(column_key, (device_total + 1,), 0, COLS)
    tile_index = jnp.arange(tiles_band)
    top_forced = tile_index[None, :] == boundary_cols[:-1, None]
    bottom_forced = tile_index[None, :] == (ROWS_DEV - 1) * COLS + boundary_cols[1:, None]
    band_index = jnp.arange(device_total)[:, None]
    forced = top_forced & (band_index > 0) | bottom_forced & (band_index < device_total - 1)
    scores = jax.random.randint(order_key, (device_total, tiles_band), 0, 1 << 20) * tiles_band
    scores = scores + tile_index[None, :]
    scores = jnp.where(forced, -1 - tile_index[None, :], scores)
    ranking = jnp.argsort(jnp.argsort(scores, axis=1), axis=1)
    tissue = (ranking < counts[:, None]).astype(jnp.int32)
    return tissue.reshape(device_total * ROWS_DEV, COLS)


def steps_of(key, dims, cuts, smallest, largest):
    loudness, own = 1.0, jax.random.fold_in(key, 6)
    for dim, parts in cuts:
        steps = jnp.exp(jax.random.uniform(jax.random.fold_in(own, dim), (parts,), jnp.float32, smallest / len(cuts), largest / len(cuts)))
        loudness = loudness * jnp.repeat(steps, dims[dim] // parts).reshape([-1 if axis == dim else 1 for axis in range(len(dims))])
    return loudness


def noise(stream_key, extent, width, bound, cuts=(), held_as=jnp.bfloat16):
    loudness = steps_of(stream_key, extent, cuts, -0.22, 0.18) if cuts else 1.0
    array = jax.random.normal(stream_key, extent, jnp.float32) * width * loudness
    return jnp.minimum(jnp.maximum(array, -bound), bound).astype(held_as)


def setup_inputs(seed: int = 0, part: int = 0) -> dict:
    key_of = jax.random.split(jax.random.key(seed), 5)
    own_keys = jax.random.split(jax.random.fold_in(key_of[4], part), 5)
    slide_pixels = noise(own_keys[0], (GRID_ROWS * SIDE, COLS * SIDE * CH), 1.0, 6.0, ((0, 16),))
    tissue_mask = draw_tissue_mask(jax.random.fold_in(jax.random.fold_in(key_of[4], part), 71), part)
    conv_weight = noise(key_of[2], (3, 3, CH, CH), (9 * CH) ** -0.5, 0.25)
    conv_bias = noise(key_of[3], (CH,), 0.5, 3.0)
    return dict(slide_pixels=slide_pixels, tissue_mask=tissue_mask, conv_weight=conv_weight, conv_bias=conv_bias)


def reference(slide_pixels, tissue_mask, conv_weight, conv_bias):
    grid_rows, grid_cols = tissue_mask.shape
    channels = conv_weight.shape[2]
    side = slide_pixels.shape[0] // grid_rows
    image = slide_pixels.reshape(grid_rows * side, grid_cols * side, channels)
    flat_mask = tissue_mask.reshape(grid_rows * grid_cols)
    order = jnp.argsort(1 - flat_mask, stable=True)[: N_ROW * SLOTS].astype(jnp.int32)
    weight_full = conv_weight.astype(jnp.float32)
    bias_full = conv_bias.astype(jnp.float32)

    def one_tile(position):
        tile_row = position // grid_cols
        tile_col = position % grid_cols
        offsets = jnp.arange(side + 2, dtype=jnp.int32) - 1
        pixel_rows = tile_row * side + offsets
        pixel_cols = tile_col * side + offsets
        row_inside = (pixel_rows >= 0) & (pixel_rows < grid_rows * side)
        col_inside = (pixel_cols >= 0) & (pixel_cols < grid_cols * side)
        rows_safe = jnp.clip(pixel_rows, 0, grid_rows * side - 1).astype(jnp.int32)
        cols_safe = jnp.clip(pixel_cols, 0, grid_cols * side - 1).astype(jnp.int32)
        window = jnp.take(jnp.take(image, rows_safe, axis=0), cols_safe, axis=1).astype(jnp.float32)
        tissue = jnp.take(jnp.take(tissue_mask, rows_safe // side, axis=0), cols_safe // side, axis=1)
        living = row_inside[:, None] & col_inside[None, :] & (tissue == 1)
        window = jnp.where(living[:, :, None], window, jnp.zeros_like(window))
        result = jnp.zeros((side, side, channels), jnp.float32)
        for vertical in range(3):
            for horizontal in range(3):
                result = result + jnp.einsum(
                    "hwc,co->hwo",
                    window[vertical:vertical + side, horizontal:horizontal + side],
                    weight_full[vertical, horizontal],
                    precision=lax.Precision.HIGHEST)
        result = result + bias_full
        return result.astype(jnp.bfloat16).reshape(side, side * channels)

    return lax.map(one_tile, order)
```

```python
import functools
import math

import jax
import jax.numpy as jnp
from jax import lax
from jax.experimental import pallas as pl
from jax.experimental.pallas import tpu as pltpu
from jax.sharding import PartitionSpec as P

SLOTS = 8
SHIFT_MOST = 2
LANES = 128
PACK = 16
GROUP = 4
MESH = pl.DeviceIdType.MESH


def kernel(
    n, side, channels,
    x_any, mask_any, w_any, b_any, out_ref,
    image, own, rows3, wide, w_ref, b_ref, mask_s,
    row_first, row_second, row_late, row_last, halo_top, halo_bot,
    onward, arrived, edge, rim_out, rim_in, tally, chain_in, group_out, group_in,
    x_sem, in_sem, halo_send, halo_recv, tile_send, tile_recv, rim_send, rim_recv,
    chain_send, chain_recv, group_send, group_recv,
):
    band_rows, cols = mask_s.shape
    height = band_rows * side
    width = side * channels
    tiles = band_rows * cols
    quad = 2 * LANES
    groups = width // quad
    per = quad // channels
    half = LANES // channels
    team = math.gcd(n, GROUP)
    me = lax.axis_index("row")
    seat = lax.rem(me, team)
    base = me - seat
    deep = lax.div(base, team)
    is_first = me == 0
    is_last = me == n - 1
    has_back = me >= team
    has_ahead = me + team < n

    barrier = pltpu.get_barrier_semaphore()

    def greet(target):
        pl.semaphore_signal(barrier, inc=1, device_id={"row": target}, device_id_type=MESH)

    for j in range(1, team):
        greet(base + lax.rem(seat + j, team))

    @pl.when(jnp.logical_and(seat == 0, jnp.logical_not(is_first)))
    def _():
        greet(me - 1)

    @pl.when(jnp.logical_and(seat == team - 1, jnp.logical_not(is_last)))
    def _():
        greet(me + 1)

    @pl.when(has_back)
    def _():
        greet(me - team)

    def fetch(r, c):
        return pltpu.make_async_copy(
            x_any.at[pl.ds(r * side, side), pl.ds(c * width, width)],
            image.at[r + 1, c + 1],
            x_sem.at[r * cols + c],
        )

    get_mask = pltpu.make_async_copy(mask_any, mask_s, in_sem.at[0])
    get_w = pltpu.make_async_copy(w_any, w_ref, in_sem.at[1])
    get_b = pltpu.make_async_copy(b_any, b_ref, in_sem.at[2])
    get_mask.start()
    get_w.start()
    get_b.start()
    for c in range(cols):
        for r in range(band_rows):
            fetch(r, c).start()

    for r in range(1, band_rows + 1):
        image[r, 0, :, width - LANES:width] = jnp.zeros((side, LANES), jnp.bfloat16)
        image[r, cols + 1, :, 0:LANES] = jnp.zeros((side, LANES), jnp.bfloat16)
    for c in range(cols + 2):
        image[0, c, side - PACK:side, :] = jnp.zeros((PACK, width), jnp.bfloat16)
        image[band_rows + 1, c, 0:PACK, :] = jnp.zeros((PACK, width), jnp.bfloat16)

    @pl.when(is_first)
    def _():
        halo_top[...] = jnp.zeros_like(halo_top)

    @pl.when(is_last)
    def _():
        halo_bot[...] = jnp.zeros_like(halo_bot)

    get_mask.wait()
    seen = []
    for r in range(band_rows):
        for c in range(cols):
            seen.append(mask_s[r, c] + (seen[-1] if seen else 0))
    count = seen[-1]

    def place(rank):
        spot = jnp.int32(0)
        row = jnp.int32(0)
        for t in range(tiles - 1):
            past = jnp.where(seen[t] <= rank, 1, 0)
            spot = spot + past
            if t % cols == cols - 1:
                row = row + past
        return row, spot - row * cols

    get_w.wait()
    none = jnp.zeros((channels, channels), jnp.bfloat16)
    for dy in range(3):
        taps = [w_ref[dy, 0], w_ref[dy, 1], w_ref[dy, 2]]
        for p in range(2 * per):
            for q in range(per // half):
                u = p - half - half * q
                parts = [taps[u + 1 - o] if 0 <= u + 1 - o <= 2 else none for o in range(half)]
                wide[dy, p * channels:(p + 1) * channels, q * LANES:(q + 1) * LANES] = (
                    jnp.concatenate(parts, axis=1)
                )
    get_b.wait()
    bias = b_ref[...].astype(jnp.float32)
    bias = jnp.concatenate([bias] * per, axis=1)

    lines = [[], [], [], []]
    for c in range(cols):
        for r in range(band_rows):
            fetch(r, c).wait()
            keep = jnp.full((side, LANES), mask_s[r, c], jnp.int32).astype(jnp.float32)
            keep = keep.astype(jnp.bfloat16)
            for k in range(width // LANES):
                at = (r + 1, c + 1, slice(None), pl.ds(k * LANES, LANES))
                image[at] = image[at] * keep
        first = image[1, c + 1, 0:PACK].astype(jnp.float32)
        last = image[band_rows, c + 1, side - PACK:side].astype(jnp.float32)
        lines[0].append(first[0:1])
        lines[1].append(first[1:2])
        lines[2].append(last[PACK - 2:PACK - 1])
        lines[3].append(last[PACK - 1:PACK])
    for ref, found in zip((row_first, row_second, row_late, row_last), lines):
        ref[...] = jnp.concatenate(found, axis=0).astype(jnp.bfloat16)

    tally[...] = jnp.full(tally.shape, count, jnp.int32)

    outside = jnp.logical_or(
        jnp.logical_and(seat == 0, jnp.logical_not(is_first)),
        jnp.logical_and(seat == team - 1, jnp.logical_not(is_last)))
    pl.semaphore_wait(
        barrier, team - 1 + jnp.where(outside, 1, 0) + jnp.where(has_ahead, 1, 0))

    ahead = {"row": lax.rem(me + 1, n)}
    behind = {"row": lax.rem(me + n - 1, n)}
    down = pltpu.make_async_remote_copy(
        row_last, halo_top, halo_send.at[0], halo_recv.at[0],
        device_id=ahead, device_id_type=MESH)
    up = pltpu.make_async_remote_copy(
        row_first, halo_bot, halo_send.at[1], halo_recv.at[1],
        device_id=behind, device_id_type=MESH)
    relay = pltpu.make_async_remote_copy(
        tally, chain_in, chain_send, chain_recv,
        device_id={"row": lax.rem(me + team, n)}, device_id_type=MESH)

    def tile(k):
        return pltpu.make_async_remote_copy(
            onward.at[k], arrived.at[k], tile_send.at[k], tile_recv.at[k],
            device_id=ahead, device_id_type=MESH)

    rims = pltpu.make_async_remote_copy(
        rim_out, rim_in, rim_send, rim_recv, device_id=ahead, device_id_type=MESH)

    def share(target, slot):
        return pltpu.make_async_remote_copy(
            group_out, group_in.at[slot], group_send.at[target], group_recv.at[slot],
            device_id={"row": base + target}, device_id_type=MESH)

    @pl.when(jnp.logical_not(is_first))
    def _():
        up.start()

    @pl.when(jnp.logical_not(is_last))
    def _():
        down.start()

    upper = lax.broadcasted_iota(jnp.int32, tally.shape, 0) < tally.shape[0] // 2

    def spread(before):
        group_out[...] = jnp.where(upper, before, tally[...])
        for j in range(1, team):
            share(lax.rem(seat + j, team), seat).start()

    @pl.when(jnp.logical_not(has_back))
    def _():
        @pl.when(has_ahead)
        def _():
            relay.start()
        spread(jnp.zeros(tally.shape, jnp.int32))

    def pass_on():
        relay.wait_recv()
        spread(chain_in[...])
        tally[...] = chain_in[...] + tally[...]

        @pl.when(has_ahead)
        def _():
            relay.start()

    def convolve(spots, put):
        for i, (r, c) in enumerate(spots):
            for k in range(width // LANES + 2):
                if k == 0:
                    at, lane = c, width - LANES
                elif k <= width // LANES:
                    at, lane = c + 1, (k - 1) * LANES
                else:
                    at, lane = c + 2, 0
                lane = slice(lane, lane + LANES)
                block = image[r + 1, at, :, lane]
                above = image[r, at, side - PACK:side, lane].astype(jnp.float32)
                below = image[r + 2, at, 0:PACK, lane].astype(jnp.float32)
                block32 = block.astype(jnp.float32)
                span = pl.ds(i * (groups + 1) * quad + k * LANES, LANES)
                rows3[0, :, span] = jnp.concatenate(
                    [above[PACK - 1:PACK], block32[0:side - 1]], axis=0).astype(jnp.bfloat16)
                rows3[1, :, span] = block
                rows3[2, :, span] = jnp.concatenate(
                    [block32[1:side], below[0:1]], axis=0).astype(jnp.bfloat16)
        starts = [(i * (groups + 1) + g) * quad for i in range(len(spots)) for g in range(groups)]
        left_side = jnp.concatenate([jnp.concatenate(
            [rows3[dy, :, s:s + 2 * quad] for s in starts], axis=0)
            for dy in range(3)], axis=1)
        total = jnp.dot(left_side, wide[...].reshape(6 * quad, quad),
            preferred_element_type=jnp.float32) + bias
        done = total.astype(jnp.bfloat16)
        for i in range(len(spots)):
            for g in range(groups):
                at = (i * groups + g) * side
                put(i, g, done[at:at + side])

    leaving = [place(count - SHIFT_MOST + k) for k in range(SHIFT_MOST)]
    for k in range(SHIFT_MOST):
        def put_onward(i, g, value, k=k):
            onward[k, :, g * quad:(g + 1) * quad] = value

        convolve([leaving[k]], put_onward)

        @pl.when(jnp.logical_not(is_last))
        def _(k=k):
            tile(k).start()

    duo = 2
    duos = SLOTS // duo
    turn = (deep - 1) * 2

    def several(j, carry):
        @pl.when(jnp.logical_and(has_back, turn == j))
        def _():
            pass_on()

        def put_own(i, g, value):
            own[j * duo + i, :, g * quad:(g + 1) * quad] = value

        convolve([place(j * duo + i) for i in range(duo)], put_own)
        return carry

    lax.fori_loop(0, duos, several, 0)

    @pl.when(jnp.logical_and(has_back, turn >= duos))
    def _():
        pass_on()

    @pl.when(jnp.logical_not(is_first))
    def _():
        down.wait_recv()

    @pl.when(jnp.logical_not(is_last))
    def _():
        up.wait_recv()

    sides = []
    for trio in ((halo_top, row_first, row_second), (row_late, row_last, halo_bot)):
        parts = []
        for ref in trio:
            line = ref[...].astype(jnp.float32)
            blank = jnp.zeros((1, LANES), jnp.float32)
            before = jnp.concatenate([blank, line[0:cols - 1, width - LANES:width]], axis=0)
            after = jnp.concatenate([line[1:cols, 0:LANES], blank], axis=0)
            line = jnp.concatenate([before, line, after], axis=1)
            parts.append(jnp.concatenate(
                [line[:, g * quad:(g + 2) * quad] for g in range(groups)], axis=0))
        sides.append(jnp.concatenate(parts, axis=1))
    rim = jnp.dot(
        jnp.concatenate(sides, axis=0).astype(jnp.bfloat16), wide[...].reshape(6 * quad, quad),
        preferred_element_type=jnp.float32) + bias
    for s in range(2):
        for g in range(groups):
            at = (s * groups + g) * cols
            for c in range(cols):
                edge[s, c, :, g * quad:(g + 1) * quad] = rim[at + c:at + c + 1]

    ends = []
    for k in range(SHIFT_MOST):
        r, c = leaving[k]
        at_top = jnp.full((1, width), r, jnp.int32) == 0
        at_end = jnp.full((1, width), r, jnp.int32) == band_rows - 1
        ends.append(jnp.where(
            at_top, edge[0, c], onward[k, 0:PACK].astype(jnp.float32)[0:1]))
        ends.append(jnp.where(
            at_end, edge[1, c],
            onward[k, side - PACK:side].astype(jnp.float32)[PACK - 1:PACK]))
    rim_out[...] = jnp.concatenate(ends, axis=0).astype(jnp.bfloat16)

    @pl.when(jnp.logical_not(is_last))
    def _():
        rims.start()

    line_at = lax.broadcasted_iota(jnp.int32, (PACK, quad), 0)

    def finish(j, carry):
        r, c = place(j)
        rows = jnp.full((PACK, quad), r, jnp.int32)
        at_top = jnp.logical_and(rows == 0, line_at == 0)
        at_end = jnp.logical_and(rows == band_rows - 1, line_at == PACK - 1)
        for g in range(groups):
            span = pl.ds(g * quad, quad)
            for s, where, at in ((0, at_top, 0), (1, at_end, side - PACK)):
                old = own[j, at:at + PACK, span].astype(jnp.float32)
                new = jnp.broadcast_to(edge[s, c, :, span], (PACK, quad))
                own[j, at:at + PACK, span] = jnp.where(where, new, old).astype(jnp.bfloat16)
        return carry

    lax.fori_loop(0, SLOTS, finish, 0)

    sum_of = group_out[...] * jnp.where(upper, 1, 0)
    for j in range(1, team):
        slot = lax.rem(seat + j, team)
        share(slot, slot).wait_recv()
        earlier = jnp.where(slot < seat, 1, 0)
        sum_of = sum_of + group_in[slot] * jnp.where(upper, 1, earlier)
    row_at = lax.broadcasted_iota(jnp.int32, tally.shape, 0)
    lane_at = lax.broadcasted_iota(jnp.int32, tally.shape, 1)
    chosen = jnp.logical_and(lane_at == 0, lax.rem(row_at, tally.shape[0] // 2) == 0)
    excess = jnp.sum(jnp.where(chosen, sum_of, 0)) - SLOTS * me

    for k in range(SHIFT_MOST, SLOTS):
        out_ref[k] = own[jnp.clip(k - excess, 0, SLOTS - 1)]

    for k in range(SHIFT_MOST):
        out_ref[k] = own[jnp.clip(k - excess, 0, SLOTS - 1)]

    @pl.when(jnp.logical_not(is_first))
    def _():
        rims.wait_recv()
        for k in range(SHIFT_MOST):
            tile(k).wait_recv()
        ends = rim_in[...].astype(jnp.float32)
        for k in range(SHIFT_MOST):
            source = jnp.minimum(
                k + SHIFT_MOST - jnp.clip(excess, 0, SHIFT_MOST), SHIFT_MOST - 1)
            late = jnp.full((PACK, quad), excess, jnp.int32) > k
            second = jnp.full((PACK, quad), source, jnp.int32) == 1
            for g in range(groups):
                span = pl.ds(g * quad, quad)
                for s, line, at in ((0, 0, 0), (1, PACK - 1, side - PACK)):
                    theirs = arrived[source, at:at + PACK, span].astype(jnp.float32)
                    end = jnp.where(
                        second,
                        jnp.broadcast_to(ends[2 + s:3 + s, g * quad:(g + 1) * quad], (PACK, quad)),
                        jnp.broadcast_to(ends[s:s + 1, g * quad:(g + 1) * quad], (PACK, quad)))
                    theirs = jnp.where(line_at == line, end, theirs)
                    mine = out_ref[k, at:at + PACK, span].astype(jnp.float32)
                    out_ref[k, at:at + PACK, span] = (
                        jnp.where(late, theirs, mine).astype(jnp.bfloat16))
        up.wait_send()

    @pl.when(jnp.logical_not(is_last))
    def _():
        down.wait_send()
        rims.wait_send()
        for k in range(SHIFT_MOST):
            tile(k).wait_send()

    @pl.when(has_ahead)
    def _():
        relay.wait_send()

    for j in range(1, team):
        share(lax.rem(seat + j, team), seat).wait_send()


def on_device(slide_pixels, tissue_mask, conv_weight, conv_bias):
    n = lax.axis_size("row")
    band_rows, cols = tissue_mask.shape
    channels = conv_weight.shape[2]
    height = slide_pixels.shape[0]
    side = height // band_rows
    width = side * channels
    quad = 2 * LANES
    team = math.gcd(n, GROUP)
    bf16 = jnp.bfloat16
    dma = pltpu.SemaphoreType.DMA
    anywhere = pl.BlockSpec(memory_space=pl.ANY)
    line = pltpu.VMEM((cols, width), bf16)
    note = pltpu.VMEM((8, LANES), jnp.int32)
    return pl.pallas_call(
        functools.partial(kernel, n, side, channels),
        out_shape=pltpu.VMEM((SLOTS, side, width), bf16),
        in_specs=[anywhere] * 4,
        out_specs=pl.BlockSpec(memory_space=pltpu.VMEM),
        scratch_shapes=[
            pltpu.VMEM((band_rows + 2, cols + 2, side, width), bf16),
            pltpu.VMEM((SLOTS, side, width), bf16),
            pltpu.VMEM((3, side, 2 * (width + quad)), bf16),
            pltpu.VMEM((3, 2 * quad, quad), bf16),
            pltpu.VMEM(conv_weight.shape, bf16),
            pltpu.VMEM((1, channels), bf16),
            pltpu.SMEM((band_rows, cols), jnp.int32),
            line, line, line, line, line, line,
            pltpu.VMEM((SHIFT_MOST, side, width), bf16),
            pltpu.VMEM((SHIFT_MOST, side, width), bf16),
            pltpu.VMEM((2, cols, 1, width), jnp.float32),
            pltpu.VMEM((2 * SHIFT_MOST, width), bf16),
            pltpu.VMEM((2 * SHIFT_MOST, width), bf16),
            note, note, note,
            pltpu.VMEM((team, 8, LANES), jnp.int32),
            dma((band_rows * cols,)), dma((3,)), dma((2,)), dma((2,)),
            dma((SHIFT_MOST,)), dma((SHIFT_MOST,)), dma, dma, dma, dma,
            dma((team,)), dma((team,)),
        ],
        compiler_params=pltpu.CompilerParams(collective_id=0, has_side_effects=True),
    )(slide_pixels, tissue_mask, conv_weight, conv_bias.reshape(1, channels))


def solution(mesh):
    return jax.shard_map(
        on_device,
        mesh=mesh,
        in_specs=(P(("slides", "row"), None), P(("slides", "row"), None), P(), P()),
        out_specs=P(("slides", "row"), None, None),
        check_vma=False,
    )
```

```python
import functools

import jax
import jax.numpy as jnp
from jax import lax
from jax.experimental import pallas as pl
from jax.experimental.pallas import tpu as pltpu
from jax.sharding import PartitionSpec as P

SLOTS = 8
SHIFT_MOST = 2
LANES = 128
PACK = 16
TEAM = 4
MESH = pl.DeviceIdType.MESH


def kernel(
    n, side, channels,
    x_any, mask_any, w_any, b_any, out_ref,
    image, own, rows3, wide, w_ref, b_ref, mask_s,
    lines, row_first, row_last, halo_top, halo_bot,
    onward, arrived, edge, below,
    top_out, top_in, end_out, end_in, pick_out, pick_in,
    tally, mate, pair, pair_in, chain_out, chain_in,
    x_sem, in_sem, halo_send, halo_recv, tile_send, tile_recv, rim_send, rim_recv,
    mate_send, mate_recv, pair_send, pair_recv, chain_send, chain_recv,
):
    band_rows, cols = mask_s.shape
    width = side * channels
    tiles = band_rows * cols
    quad = 2 * LANES
    groups = width // quad
    per = quad // channels
    half = LANES // channels
    me = lax.axis_index("row")
    seat = lax.rem(me, TEAM)
    base = me - seat
    deep = lax.div(base, TEAM)
    odd = lax.rem(me, 2) == 1
    even = jnp.logical_not(odd)
    chip = lax.div(seat, 2)
    is_first = me == 0
    is_last = me == n - 1
    has_back = me >= TEAM
    has_ahead = base + TEAM < n

    barrier = pltpu.get_barrier_semaphore()

    def greet(target):
        pl.semaphore_signal(barrier, inc=1, device_id={"row": target}, device_id_type=MESH)

    @pl.when(odd)
    def _():
        greet(me - 1)

    @pl.when(jnp.logical_not(is_last))
    def _():
        greet(me + 1)

    @pl.when(seat == 2)
    def _():
        greet(me - 1)

    @pl.when(seat == 3)
    def _():
        greet(me - 2)

    @pl.when(has_back)
    def _():
        greet(base - 1)
        greet(base - 3)

    def fetch(r, c):
        return pltpu.make_async_copy(
            x_any.at[pl.ds(r * side, side), pl.ds(c * width, width)],
            image.at[r + 1, c + 1],
            x_sem.at[r * cols + c],
        )

    get_mask = pltpu.make_async_copy(mask_any, mask_s, in_sem.at[0])
    get_w = pltpu.make_async_copy(w_any, w_ref, in_sem.at[1])
    get_b = pltpu.make_async_copy(b_any, b_ref, in_sem.at[2])
    get_mask.start()
    get_w.start()
    get_b.start()
    for c in range(cols):
        for r in range(band_rows):
            fetch(r, c).start()

    for r in range(1, band_rows + 1):
        image[r, 0, :, width - LANES:width] = jnp.zeros((side, LANES), jnp.bfloat16)
        image[r, cols + 1, :, 0:LANES] = jnp.zeros((side, LANES), jnp.bfloat16)
    for c in range(cols + 2):
        image[0, c, side - PACK:side, :] = jnp.zeros((PACK, width), jnp.bfloat16)
        image[band_rows + 1, c, 0:PACK, :] = jnp.zeros((PACK, width), jnp.bfloat16)

    @pl.when(is_first)
    def _():
        halo_top[...] = jnp.zeros_like(halo_top)

    @pl.when(is_last)
    def _():
        halo_bot[...] = jnp.zeros_like(halo_bot)

    @pl.when(even)
    def _():
        mate[...] = jnp.zeros_like(mate)

    @pl.when(seat < 2)
    def _():
        pair_in[...] = jnp.zeros_like(pair_in)

    @pl.when(jnp.logical_not(has_back))
    def _():
        chain_in[...] = jnp.zeros_like(chain_in)

    get_mask.wait()
    seen = []
    for r in range(band_rows):
        for c in range(cols):
            seen.append(mask_s[r, c] + (seen[-1] if seen else 0))
    count = seen[-1]

    def place(rank):
        spot = jnp.int32(0)
        row = jnp.int32(0)
        for t in range(tiles - 1):
            past = jnp.where(seen[t] <= rank, 1, 0)
            spot = spot + past
            if t % cols == cols - 1:
                row = row + past
        return row, spot - row * cols

    ahead = {"row": lax.rem(me + 1, n)}
    behind = {"row": lax.rem(me + n - 1, n)}

    def remote(source, target, send, recv, device):
        return pltpu.make_async_remote_copy(
            source, target, send, recv, device_id=device, device_id_type=MESH)

    tell_mate = remote(tally, mate, mate_send, mate_recv, ahead)
    down = remote(row_last, halo_top, halo_send.at[0], halo_recv.at[0], ahead)
    up = remote(row_first, halo_bot, halo_send.at[1], halo_recv.at[1], behind)
    tile = [
        remote(onward.at[k], arrived.at[k], tile_send.at[k], tile_recv.at[k], ahead)
        for k in range(SHIFT_MOST)
    ]
    rims = [
        remote(source, target, rim_send.at[i], rim_recv.at[i], ahead)
        for i, (source, target) in enumerate(
            ((top_out, top_in), (end_out, end_in), (pick_out, pick_in)))
    ]

    def tell_pair(j):
        return remote(pair, pair_in, pair_send.at[j], pair_recv, {"row": base + 2 + j})

    def relay(j, slot):
        return remote(
            chain_out, chain_in.at[slot], chain_send.at[j], chain_recv.at[slot],
            {"row": lax.rem(base + TEAM + j, n)})

    tally[...] = jnp.full(tally.shape, count, jnp.int32)

    @pl.when(even)
    def _():
        pl.semaphore_wait(barrier, 1 + jnp.where(is_first, 0, 1))
        tell_mate.start()

    get_w.wait()
    none = jnp.zeros((channels, channels), jnp.bfloat16)
    for dy in range(3):
        taps = [w_ref[dy, 0], w_ref[dy, 1], w_ref[dy, 2]]
        for p in range(2 * per):
            for q in range(per // half):
                u = p - half - half * q
                parts = [taps[u + 1 - o] if 0 <= u + 1 - o <= 2 else none for o in range(half)]
                wide[dy, p * channels:(p + 1) * channels, q * LANES:(q + 1) * LANES] = (
                    jnp.concatenate(parts, axis=1)
                )
    get_b.wait()
    bias = b_ref[...].astype(jnp.float32)
    bias = jnp.concatenate([bias] * per, axis=1)

    for c in range(cols):
        for r in range(band_rows):
            fetch(r, c).wait()
            keep = jnp.full((side, LANES), mask_s[r, c], jnp.int32).astype(jnp.float32)
            keep = keep.astype(jnp.bfloat16)
            for k in range(width // LANES):
                at = (r + 1, c + 1, slice(None), pl.ds(k * LANES, LANES))
                image[at] = image[at] * keep
        first = image[1, c + 1, 0:PACK].astype(jnp.float32)
        last = image[band_rows, c + 1, side - PACK:side].astype(jnp.float32)
        lines[0, c:c + 1, :] = first[0:1]
        lines[1, c:c + 1, :] = first[1:2]
        lines[2, c:c + 1, :] = last[PACK - 2:PACK - 1]
        lines[3, c:c + 1, :] = last[PACK - 1:PACK]
    row_first[...] = lines[0].astype(jnp.bfloat16)
    row_last[...] = lines[3].astype(jnp.bfloat16)

    @pl.when(odd)
    def _():
        pl.semaphore_wait(
            barrier, 1 + jnp.where(seat == 1, 2, 0) + jnp.where(has_ahead, TEAM, 0))

    @pl.when(jnp.logical_not(is_last))
    def _():
        down.start()

    def pass_on(before):
        chain_out[...] = before + pair[...]
        for j in range(TEAM):
            relay(j, chip).start()

    @pl.when(odd)
    def _():
        tell_mate.wait_recv()
        pair[...] = tally[...] + mate[...]

        @pl.when(seat == 1)
        def _():
            for j in range(2):
                tell_pair(j).start()

        @pl.when(jnp.logical_and(has_ahead, jnp.logical_not(has_back)))
        def _():
            pass_on(jnp.zeros(pair.shape, jnp.int32))

    @pl.when(jnp.logical_not(is_first))
    def _():
        up.start()

    def convolve(spots, put):
        for i, (r, c) in enumerate(spots):
            for k in range(width // LANES + 2):
                if k == 0:
                    at, lane = c, width - LANES
                elif k <= width // LANES:
                    at, lane = c + 1, (k - 1) * LANES
                else:
                    at, lane = c + 2, 0
                lane = slice(lane, lane + LANES)
                block = image[r + 1, at, :, lane]
                above = image[r, at, side - PACK:side, lane].astype(jnp.float32)
                beneath = image[r + 2, at, 0:PACK, lane].astype(jnp.float32)
                block32 = block.astype(jnp.float32)
                span = pl.ds(i * (groups + 1) * quad + k * LANES, LANES)
                rows3[0, :, span] = jnp.concatenate(
                    [above[PACK - 1:PACK], block32[0:side - 1]], axis=0).astype(jnp.bfloat16)
                rows3[1, :, span] = block
                rows3[2, :, span] = jnp.concatenate(
                    [block32[1:side], beneath[0:1]], axis=0).astype(jnp.bfloat16)
        starts = [(i * (groups + 1) + g) * quad for i in range(len(spots)) for g in range(groups)]
        left_side = jnp.concatenate([jnp.concatenate(
            [rows3[dy, :, s:s + 2 * quad] for s in starts], axis=0)
            for dy in range(3)], axis=1)
        total = jnp.dot(left_side, wide[...].reshape(6 * quad, quad),
            preferred_element_type=jnp.float32) + bias
        for i in range(len(spots)):
            for g in range(groups):
                at = (i * groups + g) * side
                put(i, g, total[at:at + side])

    leaving = [place(count - SHIFT_MOST + k) for k in range(SHIFT_MOST)]
    for k in range(SHIFT_MOST):
        def put_onward(i, g, value, k=k):
            span = slice(g * quad, (g + 1) * quad)
            onward[k, :, span] = value.astype(jnp.bfloat16)
            end_out[k:k + 1, span] = value[side - 1:side]

        convolve([leaving[k]], put_onward)

        @pl.when(jnp.logical_not(is_last))
        def _(k=k):
            tile[k].start()

    def stack(line):
        blank = jnp.zeros((1, LANES), jnp.float32)
        before = jnp.concatenate([blank, line[0:cols - 1, width - LANES:width]], axis=0)
        after = jnp.concatenate([line[1:cols, 0:LANES], blank], axis=0)
        line = jnp.concatenate([before, line, after], axis=1)
        return jnp.concatenate(
            [line[:, g * quad:(g + 2) * quad] for g in range(groups)], axis=0).astype(jnp.bfloat16)

    def rim(s, trio):
        found = jnp.dot(
            jnp.concatenate([stack(line) for line in trio], axis=1),
            wide[...].reshape(6 * quad, quad), preferred_element_type=jnp.float32) + bias
        for g in range(groups):
            for c in range(cols):
                edge[s, c, :, g * quad:(g + 1) * quad] = found[g * cols + c:g * cols + c + 1]

    def send_rims():
        @pl.when(jnp.logical_not(is_first))
        def _():
            down.wait_recv()

        rim(0, (halo_top[...].astype(jnp.float32), lines[0], lines[1]))
        row_at = lax.broadcasted_iota(jnp.int32, (cols, LANES), 0)
        tops, picks = [], []
        for k, (r, c) in enumerate(leaving):
            at_top = jnp.full((1, width), r, jnp.int32) == 0
            tops.append(jnp.where(
                at_top, edge[0, c], onward[k, 0:PACK].astype(jnp.float32)[0:1]))
            at_end = jnp.full((cols, LANES), r, jnp.int32) == band_rows - 1
            picks.append(jnp.where(jnp.logical_and(at_end, row_at == c), 1.0, 0.0))
        top_out[...] = jnp.concatenate(tops, axis=0).astype(jnp.bfloat16)
        pick_out[...] = jnp.concatenate(picks, axis=0).astype(jnp.bfloat16)

        @pl.when(jnp.logical_not(is_last))
        def _():
            for copy in rims:
                copy.start()

    duo = 2
    duos = SLOTS // duo
    turn = (deep - 1) * 2
    relays = jnp.logical_and(odd, jnp.logical_and(has_back, has_ahead))

    def take_and_pass():
        relay(0, chip).wait_recv()
        pass_on(chain_in[chip])

    def several(j, carry):
        @pl.when(jnp.logical_and(relays, turn == j))
        def _():
            take_and_pass()

        @pl.when(jnp.logical_and(odd, j == 1))
        def _():
            send_rims()

        def put_own(i, g, value):
            own[j * duo + i, :, g * quad:(g + 1) * quad] = value.astype(jnp.bfloat16)

        convolve([place(j * duo + i) for i in range(duo)], put_own)
        return carry

    lax.fori_loop(0, duos, several, 0)

    @pl.when(jnp.logical_and(relays, turn >= duos))
    def _():
        take_and_pass()

    @pl.when(even)
    def _():
        send_rims()

    adds = jnp.dot(stack(lines[0]), wide[2], preferred_element_type=jnp.float32)
    for g in range(groups):
        below[:, g * quad:(g + 1) * quad] = adds[g * cols:(g + 1) * cols]

    @pl.when(jnp.logical_not(is_last))
    def _():
        up.wait_recv()

    rim(1, (lines[2], lines[3], halo_bot[...].astype(jnp.float32)))

    line_at = lax.broadcasted_iota(jnp.int32, (PACK, quad), 0)

    def finish(j, carry):
        r, c = place(j)
        rows = jnp.full((PACK, quad), r, jnp.int32)
        at_top = jnp.logical_and(rows == 0, line_at == 0)
        at_end = jnp.logical_and(rows == band_rows - 1, line_at == PACK - 1)
        for g in range(groups):
            span = pl.ds(g * quad, quad)
            for s, where, at in ((0, at_top, 0), (1, at_end, side - PACK)):
                old = own[j, at:at + PACK, span].astype(jnp.float32)
                new = jnp.broadcast_to(edge[s, c, :, span], (PACK, quad))
                own[j, at:at + PACK, span] = jnp.where(where, new, old).astype(jnp.bfloat16)
        return carry

    lax.fori_loop(0, SLOTS, finish, 0)

    @pl.when(seat >= 2)
    def _():
        tell_pair(0).wait_recv()

    @pl.when(has_back)
    def _():
        for slot in range(2):
            @pl.when(jnp.logical_or(jnp.logical_not(relays), chip != slot))
            def _(slot=slot):
                relay(0, slot).wait_recv()

    excess = chain_in[0] + chain_in[1] + pair_in[...] + mate[...] - SLOTS * me
    excess32 = jnp.concatenate([excess] * (PACK // excess.shape[0]), axis=0).astype(jnp.float32)
    excess16 = excess32.astype(jnp.bfloat16)
    by_one = excess16 == jnp.bfloat16(1)
    by_two = excess16 == jnp.bfloat16(2)

    for k in range(SHIFT_MOST, SLOTS):
        for at in range(0, side, PACK):
            for lane in range(0, width, LANES):
                spot = (slice(at, at + PACK), slice(lane, lane + LANES))
                out_ref[(k,) + spot] = jnp.where(
                    by_two, own[(k - 2,) + spot],
                    jnp.where(by_one, own[(k - 1,) + spot], own[(k,) + spot]))

    @pl.when(is_first)
    def _():
        for k in range(SHIFT_MOST):
            out_ref[k] = own[k]

    @pl.when(jnp.logical_not(is_first))
    def _():
        for copy in tile + rims:
            copy.wait_recv()
        row16 = lax.broadcasted_iota(jnp.int32, (PACK, LANES), 0)
        one = excess32 == 1
        two = excess32 == 2
        for lane in range(0, width, LANES):
            span = slice(lane, lane + LANES)
            tops = top_in[:, span].astype(jnp.float32)
            for at, line in ((0, 0), (side - PACK, PACK - 1)):
                theirs = []
                for k in range(SHIFT_MOST):
                    if at == 0:
                        rim_row = tops[k:k + 1]
                    else:
                        pick = pick_in[...].astype(jnp.float32)[k * cols:(k + 1) * cols]
                        rim_row = end_in[k:k + 1, span] + jnp.sum(
                            pick * below[:, span], axis=0, keepdims=True)
                    theirs.append(jnp.where(
                        row16 == line, jnp.broadcast_to(rim_row, (PACK, LANES)),
                        arrived[k, at:at + PACK, span].astype(jnp.float32)))
                mine = [own[k, at:at + PACK, span].astype(jnp.float32) for k in range(SHIFT_MOST)]
                out_ref[0, at:at + PACK, span] = jnp.where(
                    two, theirs[0], jnp.where(one, theirs[1], mine[0])).astype(jnp.bfloat16)
                out_ref[1, at:at + PACK, span] = jnp.where(
                    two, theirs[1], jnp.where(one, mine[0], mine[1])).astype(jnp.bfloat16)
        up.wait_send()

    @pl.when(jnp.logical_not(is_last))
    def _():
        down.wait_send()
        for copy in tile + rims:
            copy.wait_send()

    @pl.when(even)
    def _():
        tell_mate.wait_send()

    @pl.when(seat == 1)
    def _():
        for j in range(2):
            tell_pair(j).wait_send()

    @pl.when(jnp.logical_and(odd, has_ahead))
    def _():
        for j in range(TEAM):
            relay(j, chip).wait_send()


def on_device(slide_pixels, tissue_mask, conv_weight, conv_bias):
    n = lax.axis_size("row")
    band_rows, cols = tissue_mask.shape
    channels = conv_weight.shape[2]
    height = slide_pixels.shape[0]
    side = height // band_rows
    width = side * channels
    quad = 2 * LANES
    bf16 = jnp.bfloat16
    f32 = jnp.float32
    dma = pltpu.SemaphoreType.DMA
    anywhere = pl.BlockSpec(memory_space=pl.ANY)
    line = pltpu.VMEM((cols, width), bf16)
    note = pltpu.VMEM((8, LANES), jnp.int32)
    return pl.pallas_call(
        functools.partial(kernel, n, side, channels),
        out_shape=pltpu.VMEM((SLOTS, side, width), bf16),
        in_specs=[anywhere] * 4,
        out_specs=pl.BlockSpec(memory_space=pltpu.VMEM),
        scratch_shapes=[
            pltpu.VMEM((band_rows + 2, cols + 2, side, width), bf16),
            pltpu.VMEM((SLOTS, side, width), bf16),
            pltpu.VMEM((3, side, 2 * (width + quad)), bf16),
            pltpu.VMEM((3, 2 * quad, quad), bf16),
            pltpu.VMEM(conv_weight.shape, bf16),
            pltpu.VMEM((1, channels), bf16),
            pltpu.SMEM((band_rows, cols), jnp.int32),
            pltpu.VMEM((4, cols, width), f32),
            line, line, line, line,
            pltpu.VMEM((SHIFT_MOST, side, width), bf16),
            pltpu.VMEM((SHIFT_MOST, side, width), bf16),
            pltpu.VMEM((2, cols, 1, width), f32),
            pltpu.VMEM((cols, width), f32),
            pltpu.VMEM((SHIFT_MOST, width), bf16),
            pltpu.VMEM((SHIFT_MOST, width), bf16),
            pltpu.VMEM((SHIFT_MOST, width), f32),
            pltpu.VMEM((SHIFT_MOST, width), f32),
            pltpu.VMEM((SHIFT_MOST * cols, LANES), bf16),
            pltpu.VMEM((SHIFT_MOST * cols, LANES), bf16),
            note, note, note, note, note,
            pltpu.VMEM((2, 8, LANES), jnp.int32),
            dma((band_rows * cols,)), dma((3,)), dma((2,)), dma((2,)),
            dma((SHIFT_MOST,)), dma((SHIFT_MOST,)), dma((3,)), dma((3,)),
            dma, dma, dma((2,)), dma, dma((TEAM,)), dma((2,)),
        ],
        compiler_params=pltpu.CompilerParams(collective_id=0, has_side_effects=True),
    )(slide_pixels, tissue_mask, conv_weight, conv_bias.reshape(1, channels))


def solution(mesh):
    return jax.shard_map(
        on_device,
        mesh=mesh,
        in_specs=(P(("slides", "row"), None), P(("slides", "row"), None), P(), P()),
        out_specs=P(("slides", "row"), None, None),
        check_vma=False,
    )
```
